256 devices in a mesh: tiles: 4 (over y, x), slab: 64 (over z, core).
Axes of the slice: x: 2, y: 2, z: 32, core: 2. Of those that a mesh axis runs over, the one named last changes fastest.
The devices are a block of a 4x8x32 slice.
Arguments:
- transmission: float32 [16384, 4096], P(('tiles', 'slab')), parts along dimension 0, may hold values from -6 to 6
- kernel_spectra: float32 [12, 2, 256, 256], replicated, may hold values from -6 to 6
Outputs:
- resist_image: float32 [16384, 256], P(('tiles', 'slab')), parts along dimension 0
The draws below stay inside these ranges and needn't reach their ends.
There are 4 independent parts, one for each index of `tiles`. The reference program is written for one: setup_inputs(seed, part) draws one part's arguments, and reference() takes and returns one part's arrays. A program takes and returns all parts, laid end to end along the dimension named above; an argument that names none is the same for every part. Nothing has to cross between parts.
All inputs are finite; a program needn't handle non-finite values.
Results may differ from the reference program's by a relative error of at most 0.0001.
Values sent between devices are 32-bit elements; how exact they have to be, the bound alone decides.
A program may use at most 128 MiB of HBM per device.

```python
import math
import jax
import jax.numpy as jnp
from jax import lax

N = 4096
B = 256
NK = 12
COLS = 256


def shard_levels(own_key, shape, shards, least, high):
    factor_of = 1.0
    for dim, shards_of in shards:
        heights = jax.random.uniform(jax.random.fold_in(jax.random.fold_in(own_key, 6), dim), (shards_of,), jnp.float32, least / len(shards), high / len(shards))
        factor_of = factor_of * jnp.repeat(jnp.exp(heights), shape[dim] // shards_of).reshape((-1,) + (1,) * (len(shape) - 1 - dim))
    return factor_of


def scatter_about(stream_key, dims, deviation, limit, split=(), kind=jnp.bfloat16):
    loudness = shard_levels(stream_key, dims, split, -0.22, 0.18) if split else 1.0
    entries = jax.random.normal(stream_key, dims, jnp.float32) * deviation * loudness
    return jnp.minimum(jnp.maximum(entries, -limit), limit).astype(kind)


def setup_inputs(seed: int = 0, part: int = 0) -> dict:
    arg_keys = jax.random.split(jax.random.key(seed), 3)
    part_splits = jax.random.split(jax.random.fold_in(arg_keys[2], part), 3)
    return {
        "transmission": scatter_about(part_splits[0], (N, N), 1.0, 6.0, ((0, 64),), jnp.float32),
        "kernel_spectra": scatter_about(arg_keys[1], (NK, 2, B, B), 1.0, 6.0, (), jnp.float32),
    }


binomial = (0.0625, 0.25, 0.375, 0.25, 0.0625)


def phase_tables(positions, tile_side, band_size):
    frequency = jnp.arange(band_size, dtype=jnp.int32) - band_size // 2
    residue = jnp.mod(positions[:, None] * frequency[None, :], tile_side)
    angles = residue.astype(jnp.float32) * (2.0 * math.pi / tile_side)
    return jnp.cos(angles), jnp.sin(angles)


def product(left, right):
    return jnp.dot(left, right, precision=lax.Precision.HIGHEST, preferred_element_type=jnp.float32)


def contract_first(left, right):
    return lax.dot_general(left, right, (((0,), (0,)), ((), ())), precision=lax.Precision.HIGHEST, preferred_element_type=jnp.float32)


def contract_last(left, right):
    return lax.dot_general(left, right, (((1,), (1,)), ((), ())), precision=lax.Precision.HIGHEST, preferred_element_type=jnp.float32)


def kernel_intensity(row_cosine, row_sine, cosine_table, sine_table, spectrum_real, spectrum_imag, kernel_spectra, norm_factor):
    half_rows = row_cosine.shape[0]

    def accumulate(running, kernel):
        prod_real = (kernel[0] * spectrum_real - kernel[1] * spectrum_imag) * norm_factor
        prod_imag = (kernel[0] * spectrum_imag + kernel[1] * spectrum_real) * norm_factor
        left_real = product(row_cosine, prod_real) - product(row_sine, prod_imag)
        left_imag = product(row_cosine, prod_imag) + product(row_sine, prod_real)
        stacked = jnp.concatenate([left_real, left_imag], 0)
        with_cosine = contract_last(stacked, cosine_table)
        with_sine = contract_last(stacked, sine_table)
        field_real = with_cosine[:half_rows] - with_sine[half_rows:]
        field_imag = with_sine[:half_rows] + with_cosine[half_rows:]
        return running + field_real * field_real + field_imag * field_imag, None

    start = jnp.zeros((half_rows, cosine_table.shape[0]), jnp.float32)
    running, unused = lax.scan(accumulate, start, kernel_spectra)
    return running / kernel_spectra.shape[0]


def reference(transmission, kernel_spectra):
    tile_side = transmission.shape[1]
    band_size = kernel_spectra.shape[2]
    cosine_table, sine_table = phase_tables(jnp.arange(tile_side, dtype=jnp.int32), tile_side, band_size)
    window_positions = jnp.mod(jnp.arange(COLS + 4, dtype=jnp.int32) - 2, tile_side).astype(jnp.int32)
    out_cosine, out_sine = phase_tables(window_positions, tile_side, band_size)
    column_real = product(transmission, cosine_table)
    column_imag = -product(transmission, sine_table)
    spectrum_real = contract_first(cosine_table, column_real) + contract_first(sine_table, column_imag)
    spectrum_imag = contract_first(cosine_table, column_imag) - contract_first(sine_table, column_real)
    norm_factor = 1.0 / (tile_side * band_size)
    intensity = kernel_intensity(cosine_table, sine_table, out_cosine, out_sine, spectrum_real, spectrum_imag, kernel_spectra, norm_factor)
    row_blurred = jnp.zeros_like(intensity)
    for position, weight in enumerate(binomial):
        row_blurred = row_blurred + weight * jnp.roll(intensity, 2 - position, axis=0)
    resist_image = jnp.zeros((tile_side, COLS), jnp.float32)
    for position, weight in enumerate(binomial):
        resist_image = resist_image + weight * row_blurred[:, position:position + COLS]
    return resist_image
```

```python
import functools
import math

import jax
import jax.numpy as jnp
import numpy as np
from jax import lax
from jax.experimental import pallas as pl
from jax.experimental.pallas import tpu as pltpu
from jax.sharding import PartitionSpec as P

COLS = 256
MESH = pl.DeviceIdType.MESH
F32, BF16 = jnp.float32, jnp.bfloat16
LANES, TILE = 128, 8
SPLIT_ROW = 24

binomial = (0.0625, 0.25, 0.375, 0.25, 0.0625)


def split(x):
    high = x.astype(BF16)
    return high, (x - high.astype(F32)).astype(BF16)


def dot(a, b):
    return lax.dot_general(a, b, (((1,), (0,)), ((), ())), preferred_element_type=F32)


def dot_t(a, b):
    return lax.dot_general(a, b, (((1,), (1,)), ((), ())), preferred_element_type=F32)


def image_kernel(
    sizes,
    t_ref, k_hbm, wy_h, wy_l, tw_chunk, w2_h, w2_l, tw_slab, e_local, ey_h, ey_l, fold, fold_t,
    out_ref,
    k_raw, k_fold, k_row, k_col, k_zero, t_h, t_l, z_ref, slots, part, pair, far, gath,
    e_h, e_l, l_zero, p_zero, q_h, q_l, acc,
    k_sem, s1, r1, s2, r2, s3, r3, sf, rf, rel,
):
    slabs, side, band, nk, rows = sizes
    half = band // 2
    blocks = half // TILE
    near = blocks // 2
    norm = 1.0 / (side * band)

    me = lax.axis_index("slab")
    chip, core = lax.div(me, 2), lax.rem(me, 2)
    own = 2 * lax.rem(chip, near) + core

    def at(step, other=False):
        where = lax.rem(me + 2 * step + slabs, slabs)
        return where + 1 - 2 * core if other else where

    def residue(step, other=False):
        c = 1 - core if other else core
        return 2 * lax.rem(chip + step + slabs, near) + c

    load = pltpu.make_async_copy(k_hbm, k_raw, k_sem)
    load.start()

    barrier = pltpu.get_barrier_semaphore()
    reach = near // 2
    count = 0
    for step in range(-reach, reach + 1):
        for other in (False, True):
            if step or other:
                pl.semaphore_signal(
                    barrier, inc=1, device_id={"slab": at(step, other)}, device_id_type=MESH
                )
                count += 1

    chunks = side // band
    group = 4
    sum_c = jnp.zeros((rows, half), F32)
    sum_s = jnp.zeros((rows, half), F32)
    row_sum = jnp.zeros((rows, LANES), F32)
    for g in range(chunks // group):
        for j in range(group):
            h = g * group + j
            piece = t_ref[:, h * band : (h + 1) * band]
            high, low = split(piece)
            t_h[h * rows : (h + 1) * rows, :] = high
            t_l[h * rows : (h + 1) * rows, :] = low
            row_sum = row_sum + piece[:, :half] + piece[:, half:]
        lo, hi = g * group * rows, (g + 1) * group * rows
        a_h, a_l = t_h[lo:hi, :], t_l[lo:hi, :]
        y = dot(a_h, wy_h[...]) + dot(a_l, wy_h[...]) + dot(a_h, wy_l[...])
        for j in range(group):
            h = g * group + j
            c = y[j * rows : (j + 1) * rows, :half]
            s = y[j * rows : (j + 1) * rows, half:]
            tc, ts = tw_chunk[h : h + 1, :half], tw_chunk[h : h + 1, half:]
            sum_c = sum_c + (c * tc - s * ts)
            sum_s = sum_s + (c * ts + s * tc)
    turned = jnp.transpose(jnp.concatenate([sum_c, sum_s], axis=0))
    column = jnp.sum(row_sum, axis=1, keepdims=True)
    lane = lax.broadcasted_iota(jnp.int32, (rows, LANES), 1)
    row = lax.broadcasted_iota(jnp.int32, (rows, LANES), 0)
    zero_row = jnp.sum(jnp.where(lane == row, column, 0.0), axis=0, keepdims=True)
    z_ref[:, 0:TILE, :] = turned.reshape(blocks, TILE, LANES)
    z_ref[:, TILE : 2 * TILE, :] = jnp.broadcast_to(zero_row[None], (blocks, TILE, LANES))

    pl.semaphore_wait(barrier, count)

    first = []
    for step in sorted(range(1 - reach, reach + 1), key=lambda d: -abs(d)):
        for other in (False, True):
            if not (step or other):
                continue
            n = len(first)
            copy = pltpu.make_async_remote_copy(
                src_ref=z_ref.at[residue(step, other), pl.ds(0, TILE + 1)],
                dst_ref=slots.at[2 * (reach - step) + core, pl.ds(0, TILE + 1)],
                send_sem=s1.at[n],
                recv_sem=r1.at[n],
                device_id={"slab": at(step, other)},
                device_id_type=MESH,
            )
            copy.start()
            first.append(copy)
    pl.semaphore_signal(rel, inc=1, device_id={"slab": at(-reach)}, device_id_type=MESH)

    slots[2 * reach + core] = z_ref[own]

    own_tw = tw_slab[pl.ds(me, 1), :]
    c0, s0 = own_tw[:, :half], own_tw[:, half:]
    ce, se = e_local[:, :half], e_local[:, half:]
    e_own = jnp.concatenate([ce * c0 - se * s0, se * c0 + ce * s0], axis=1)
    high, low = split(e_own)
    e_h[...] = high
    e_l[...] = low

    base = tw_slab[pl.ds(lax.rem(2 * (chip - reach) + slabs, slabs), 1), :]
    bc, bs = base[:, :half], base[:, half:]
    sc, ss = tw_slab[0:blocks, :half], tw_slab[0:blocks, half:]
    wc, ws = bc * sc - bs * ss, bc * ss + bs * sc

    load.wait()
    for copy in first:
        copy.wait_recv()

    k_zero[...] = jnp.zeros_like(k_zero)
    everything = slots[...]
    a_h, a_l = split(everything.reshape(blocks * 2 * TILE, LANES))
    y = dot(a_h, w2_h[...]) + dot(a_l, w2_h[...]) + dot(a_h, w2_l[...])
    cc = jnp.zeros((2 * TILE, half), F32)
    cs = jnp.zeros((2 * TILE, half), F32)
    sc2 = jnp.zeros((TILE, half), F32)
    ss2 = jnp.zeros((TILE, half), F32)
    total = jnp.zeros((2 * TILE, LANES), F32)
    for s in range(blocks):
        lo = s * 2 * TILE
        c, n = y[lo : lo + 2 * TILE, :half], y[lo : lo + 2 * TILE, half:band]
        c2, n2 = y[lo : lo + TILE, band : band + half], y[lo : lo + TILE, band + half :]
        tc, ts = wc[s : s + 1], ws[s : s + 1]
        cc = cc + (c * tc - n * ts)
        cs = cs + (c * ts + n * tc)
        sc2 = sc2 + (c2 * tc - n2 * ts)
        ss2 = ss2 + (c2 * ts + n2 * tc)
        total = total + everything[s]
    lane = lax.broadcasted_iota(jnp.int32, (TILE, LANES), 1)
    row = lax.broadcasted_iota(jnp.int32, (TILE, LANES), 0)
    left = lane < rows
    col_c = jnp.sum(jnp.where(left, total[:TILE], 0.0), axis=1, keepdims=True)
    col_s = jnp.sum(jnp.where(left, 0.0, total[:TILE]), axis=1, keepdims=True)
    both = jnp.sum(jnp.where(left, total[TILE:], 0.0), axis=1, keepdims=True)
    spot = lane == row + TILE * own
    row_c = jnp.sum(jnp.where(spot, col_c, 0.0), axis=0, keepdims=True)
    row_s = jnp.sum(jnp.where(spot, col_s, 0.0), axis=0, keepdims=True)
    extra = jnp.where(row == 0, row_c, 0.0)
    extra = jnp.where(row == 1, row_s, extra)
    extra = jnp.where(row == 2, cc[TILE : TILE + 1], extra)
    extra = jnp.where(row == 3, cs[TILE : TILE + 1], extra)
    extra = jnp.where(row == 4, both[0:1], extra)
    part[0:8, :] = cc[:TILE]
    part[8:16, :] = cs[:TILE]
    part[16:24, :] = sc2
    part[24:32, :] = ss2
    part[32:40, :] = extra

    pl.semaphore_wait(rel, 1)
    second = []
    for i, step in enumerate((near, -near)):
        copy = pltpu.make_async_remote_copy(
            src_ref=part,
            dst_ref=pair.at[i],
            send_sem=s2.at[i],
            recv_sem=r2.at[i],
            device_id={"slab": at(step)},
            device_id_type=MESH,
        )
        copy.start()
        second.append(copy)

    onehot = (lax.broadcasted_iota(jnp.int32, (TILE, band), 1) == half).astype(BF16)
    lane1 = lax.broadcasted_iota(jnp.int32, (1, LANES), 1)

    def fold_one(k, carry):
        for c in range(2):
            plane = k_raw[k, c]
            p_h, p_l = split(plane)
            v_h, v_l = split(dot(fold[...], p_h) + dot(fold[...], p_l))
            u = dot(v_h, fold_t[...]) + dot(v_l, fold_t[...])
            pp, pm = u[:half, :half], u[:half, half:]
            mp, mm = u[half:, :half], u[half:, half:]
            k_fold[k, c] = pp + mm
            k_fold[k, 2 + c] = pp - mm
            k_fold[k, 4 + c] = mp + pm
            k_fold[k, 6 + c] = mp - pm
            mid = k_raw[k, c, half : half + TILE, :]
            m_h, m_l = split(mid)
            k_row[c, pl.ds(k, 1), :] = (dot(m_h, fold_t[...]) + dot(m_l, fold_t[...]))[0:1]
            n_h, n_l = split(dot_t(onehot, p_h) + dot_t(onehot, p_l))
            k_col[c, pl.ds(k, 1), :] = (dot(n_h, fold_t[...]) + dot(n_l, fold_t[...]))[0:1]
            k_zero[c, 0:1, :] = k_zero[c, 0:1, :] + jnp.where(lane1 == k, mid[0:1, half : half + 1], 0.0)
        return carry

    lax.fori_loop(0, nk // 2, fold_one, 0)

    spans = ((0, SPLIT_ROW), (SPLIT_ROW, 5 * TILE - SPLIT_ROW))
    for i, step in enumerate((near, -near)):
        second[i].wait_recv()
        copy = pltpu.make_async_remote_copy(
            src_ref=pair.at[i, pl.ds(*spans[i])],
            dst_ref=far.at[pl.ds(*spans[i])],
            send_sem=s2.at[2 + i],
            recv_sem=r2.at[2 + i],
            device_id={"slab": at(step)},
            device_id_type=MESH,
        )
        copy.start()
        second.append(copy)

    lax.fori_loop(nk // 2, nk, fold_one, 0)

    second[2].wait_recv()
    second[3].wait_recv()
    block = (((part[...] + pair[0]) + pair[1]) + far[...]) * norm
    gath[own] = block

    third, across = [], []

    def cross(slot):
        n = len(across)
        copy = pltpu.make_async_remote_copy(
            src_ref=gath.at[slot, pl.ds(0, 34)],
            dst_ref=gath.at[slot, pl.ds(0, 34)],
            send_sem=sf.at[n],
            recv_sem=rf.at[n],
            device_id={"slab": at(0, True)},
            device_id_type=MESH,
        )
        copy.start()
        across.append(copy)

    order = sorted((d for d in range(1 - reach, reach + 1) if d), key=lambda d: -abs(d))
    for i, step in enumerate(order):
        copy = pltpu.make_async_remote_copy(
            src_ref=gath.at[own, pl.ds(0, 34)],
            dst_ref=gath.at[own, pl.ds(0, 34)],
            send_sem=s3.at[i],
            recv_sem=r3.at[i],
            device_id={"slab": at(step)},
            device_id_type=MESH,
        )
        copy.start()
        third.append(copy)
    cross(own)

    r0, i0, s00 = block[34:35], -block[35:36], block[36:37]
    e_hi, e_lo = e_h[...], e_l[...]
    ur, ui = (k_col[c, :, :half] + k_col[c, :, half:] for c in range(2))
    vr, vi = (k_col[c, :, :half] - k_col[c, :, half:] for c in range(2))
    columns = (
        jnp.concatenate([ur * r0 - vi * i0, -(vi * r0 + ur * i0)], axis=1),
        jnp.concatenate([ui * r0 + vr * i0, vr * r0 - ui * i0], axis=1),
    )
    for c in range(2):
        p_h, p_l = split(columns[c])
        l0 = dot_t(e_hi, p_h) + dot_t(e_lo, p_h) + dot_t(e_hi, p_l)
        l0 = l0 + (k_zero[c, 0:1, :] * s00)[:, : l0.shape[1]]
        for k in range(nk):
            l_zero[k, c] = jnp.broadcast_to(l0[:, k : k + 1], l_zero.shape[2:])

    for i in reversed(range(len(order))):
        third[i].wait_recv()
        cross(residue(-order[i]))
    for copy in across:
        copy.wait_recv()

    planes = [gath[:, i * TILE : (i + 1) * TILE, :].reshape(half, half) for i in range(4)]
    re1 = jnp.transpose(planes[0] - planes[3])
    im1 = -jnp.transpose(planes[1] + planes[2])
    re2 = jnp.transpose(planes[0] + planes[3])
    im2 = jnp.transpose(planes[1] - planes[2])
    edges = jnp.sum(gath[:, 4 * TILE : 5 * TILE, :], axis=0)
    r0, i0 = edges[0:1], -edges[1:2]
    ur, ui = (k_row[c, :, :half] + k_row[c, :, half:] for c in range(2))
    vr, vi = (k_row[c, :, :half] - k_row[c, :, half:] for c in range(2))
    p_zero[0] = jnp.concatenate([ur * r0 - vi * i0, -(vi * r0 + ur * i0)], axis=1)
    p_zero[1] = jnp.concatenate([ui * r0 + vr * i0, vr * r0 - ui * i0], axis=1)
    acc[...] = jnp.zeros_like(acc)
    high_rows = e_h.shape[0]

    def one_kernel(k, carry):
        ur1, ui1, vr1, vi1 = k_fold[k, 0], k_fold[k, 1], k_fold[k, 2], k_fold[k, 3]
        ur2, ui2, vr2, vi2 = k_fold[k, 4], k_fold[k, 5], k_fold[k, 6], k_fold[k, 7]
        a1r, a1i = ur1 * re1 - vi1 * im1, ui1 * re1 + vr1 * im1
        a2r, a2i = ur2 * re2 - vi2 * im2, ui2 * re2 + vr2 * im2
        b1r, b1i = vr1 * re1 - ui1 * im1, vi1 * re1 + ur1 * im1
        b2r, b2i = vr2 * re2 - ui2 * im2, vi2 * re2 + ur2 * im2
        places = (
            (0, 0, a1r + a2r), (0, half, -(b1i + b2i)), (half, 0, b2i - b1i), (half, half, a2r - a1r),
            (0, band, a1i + a2i), (0, band + half, b1r + b2r), (half, band, b1r - b2r),
            (half, band + half, a2i - a1i),
        )
        for r, c, value in places:
            high, low = split(value)
            q_h[r : r + half, c : c + half] = high
            q_l[r : r + half, c : c + half] = low
        w = dot(e_h[...], q_h[...]) + dot(e_l[...], q_h[...]) + dot(e_h[...], q_l[...])
        l_re = w[:, :band] + p_zero[0, pl.ds(k, 1), :]
        l_im = w[:, band:] + p_zero[1, pl.ds(k, 1), :]
        l_h, l_l = split(jnp.concatenate([l_re, l_im], axis=0))
        f = dot(l_h, ey_h[...]) + dot(l_l, ey_h[...]) + dot(l_h, ey_l[...])
        for i in range(acc.shape[1] // LANES):
            at_lanes = slice(i * LANES, (i + 1) * LANES)
            f_re = f[:high_rows, at_lanes] + l_zero[k, 0]
            f_im = f[high_rows:, at_lanes] + l_zero[k, 1]
            acc[:, at_lanes] = acc[:, at_lanes] + (f_re * f_re + f_im * f_im)
        return carry

    lax.fori_loop(0, nk, one_kernel, 0)

    down = sum(w * acc[i : i + rows, :] for i, w in enumerate(binomial))
    image = sum(w * down[:, i : i + COLS] for i, w in enumerate(binomial))
    out_ref[...] = image * (1.0 / nk)

    for copy in first + second + third + across:
        copy.wait_send()


def tables(slabs, side, band, rows, dtype=np.float32):
    half = band // 2
    f = np.arange(1, half + 1)

    def waves(positions):
        angle = (2.0 * math.pi / side) * np.mod(np.outer(positions, f), side)
        return np.concatenate([np.cos(angle), np.sin(angle)], axis=1)

    def halves(x):
        high = x.astype(np.float32).astype(BF16)
        return high, (x - high.astype(np.float64)).astype(BF16)

    local_w = waves(np.arange(band))
    w2 = np.zeros((2 * rows, 2 * band))
    w2[:rows, :band] = local_w[:rows]
    w2[rows:, band:] = local_w[:rows]
    edge_rows = -(-(rows + 4) // 8) * 8
    columns = np.zeros((band, -(-(COLS + 4) // LANES) * LANES))
    columns[:, : COLS + 4] = waves(np.arange(COLS + 4) - 2).T
    fold = np.zeros((band, band), np.float32)
    for i in range(half):
        if i + 1 < half:
            fold[i, half + 1 + i] = 1.0
        fold[half + i, half - 1 - i] = 1.0
    return (
        *halves(local_w),
        waves(band * np.arange(side // band)).astype(np.float32),
        *halves(w2),
        waves(rows * np.arange(slabs)).astype(np.float32),
        waves(np.arange(edge_rows) - 2).astype(np.float32),
        *halves(columns),
        fold.astype(BF16),
        fold.T.astype(BF16),
    )


def local(transmission, kernel_spectra):
    rows, side = transmission.shape
    nk, _, band, _ = kernel_spectra.shape
    slabs = lax.axis_size("slab")
    half = band // 2
    blocks = half // TILE
    constants = tables(slabs, side, band, rows)
    edge_rows = constants[6].shape[0]
    wide = constants[7].shape[1]
    nk_pad = -(-nk // 8) * 8
    vmem = pl.BlockSpec(memory_space=pltpu.VMEM)
    sends1, sends3 = blocks - 1, blocks // 2 - 1
    dma = pltpu.SemaphoreType.DMA
    return pl.pallas_call(
        functools.partial(image_kernel, (slabs, side, band, nk, rows)),
        out_shape=jax.ShapeDtypeStruct((rows, COLS), F32),
        in_specs=[vmem, pl.BlockSpec(memory_space=pl.ANY)] + [vmem] * len(constants),
        out_specs=vmem,
        scratch_shapes=[
            pltpu.VMEM(kernel_spectra.shape, F32),
            pltpu.VMEM((nk, 8, half, half), F32),
            pltpu.VMEM((2, nk_pad, band), F32),
            pltpu.VMEM((2, nk_pad, band), F32),
            pltpu.VMEM((2, TILE, LANES), F32),
            pltpu.VMEM((rows * side // band, band), BF16),
            pltpu.VMEM((rows * side // band, band), BF16),
            pltpu.VMEM((blocks, 2 * TILE, LANES), F32),
            pltpu.VMEM((blocks, 2 * TILE, LANES), F32),
            pltpu.VMEM((5 * TILE, LANES), F32),
            pltpu.VMEM((2, 5 * TILE, LANES), F32),
            pltpu.VMEM((5 * TILE, LANES), F32),
            pltpu.VMEM((blocks, 5 * TILE, LANES), F32),
            pltpu.VMEM((edge_rows, band), BF16),
            pltpu.VMEM((edge_rows, band), BF16),
            pltpu.VMEM((nk, 2, edge_rows, LANES), F32),
            pltpu.VMEM((2, nk_pad, band), F32),
            pltpu.VMEM((band, 2 * band), BF16),
            pltpu.VMEM((band, 2 * band), BF16),
            pltpu.VMEM((edge_rows, wide), F32),
            dma(()),
            dma((sends1,)),
            dma((sends1,)),
            dma((4,)),
            dma((4,)),
            dma((sends3,)),
            dma((sends3,)),
            dma((sends3 + 1,)),
            dma((sends3 + 1,)),
            pltpu.SemaphoreType.REGULAR,
        ],
        compiler_params=pltpu.CompilerParams(
            collective_id=0, has_side_effects=True, vmem_limit_bytes=60 * 1024 * 1024
        ),
        name="aerial_image",
    )(transmission, kernel_spectra, *constants)


def solution(mesh):
    return jax.shard_map(
        local,
        mesh=mesh,
        in_specs=(P(("tiles", "slab"), None), P()),
        out_specs=P(("tiles", "slab"), None),
        check_vma=False,
    )
```

```python
import functools
import math

import jax
import jax.numpy as jnp
import numpy as np
from jax import lax
from jax.experimental import pallas as pl
from jax.experimental.pallas import tpu as pltpu
from jax.sharding import PartitionSpec as P

COLS = 256
MESH = pl.DeviceIdType.MESH
F32, BF16 = jnp.float32, jnp.bfloat16
LANES, TILE = 128, 8
SPLIT_ROW, PART_ROWS = 24, 37

binomial = (0.0625, 0.25, 0.375, 0.25, 0.0625)


def split(x):
    high = x.astype(BF16)
    return high, (x - high.astype(F32)).astype(BF16)


def dot(a, b):
    return lax.dot_general(a, b, (((1,), (0,)), ((), ())), preferred_element_type=F32)


def dot_t(a, b):
    return lax.dot_general(a, b, (((1,), (1,)), ((), ())), preferred_element_type=F32)


def image_kernel(
    sizes,
    t_hbm, k_hbm, plain_hbm, near_hbm, half_hbm, wide_hbm,
    out_ref,
    t_ref, plain, near_w, halves_w, wide_w,
    k_raw, k_fold, k_row, k_col, k_zero, t_h, t_l, z_ref, slots, part, pair, far, gath,
    e_h, e_l, l_zero, p_zero, q_h, q_l, l_h, l_l, acc,
    in_sem, t_sem, s1, r1, s2, r2, s3, r3, sf, rf, rel,
):
    slabs, side, band, nk, rows = sizes
    half = band // 2
    blocks = half // TILE
    near = blocks // 2
    norm = 1.0 / (side * band)

    me = lax.axis_index("slab")
    chip, core = lax.div(me, 2), lax.rem(me, 2)
    own = 2 * lax.rem(chip, near) + core

    def at(step, other=False):
        where = lax.rem(me + 2 * step + slabs, slabs)
        return where + 1 - 2 * core if other else where

    def residue(step, other=False):
        c = 1 - core if other else core
        return 2 * lax.rem(chip + step + slabs, near) + c

    barrier = pltpu.get_barrier_semaphore()
    reach = near // 2
    count = 0
    for step in range(-reach, reach + 1):
        for other in (False, True):
            if step or other:
                pl.semaphore_signal(
                    barrier, inc=1, device_id={"slab": at(step, other)}, device_id_type=MESH
                )
                count += 1

    chunks = side // band
    group = 4
    span = group * band
    loads = [
        pltpu.make_async_copy(a, b, in_sem.at[i])
        for i, (a, b) in enumerate(
            ((near_hbm, near_w), (plain_hbm, plain), (half_hbm, halves_w), (wide_hbm, wide_w), (k_hbm, k_raw))
        )
    ]
    pieces = [
        pltpu.make_async_copy(
            t_hbm.at[:, pl.ds(g * span, span)], t_ref.at[:, pl.ds(g * span, span)], t_sem.at[g]
        )
        for g in range(chunks // group)
    ]
    for copy in pieces[:1] + loads[:2] + pieces[1:] + loads[2:]:
        copy.start()
    tw_chunk = plain.at[0:chunks]
    tw_slab = plain.at[chunks : chunks + slabs]
    e_local = plain.at[chunks + slabs :]
    wy_h, wy_l = near_w.at[0:band], near_w.at[band:]
    w2_h, w2_l = halves_w.at[0 : 2 * rows], halves_w.at[2 * rows : 4 * rows]
    fold, fold_t = halves_w.at[4 * rows : 4 * rows + band, 0:band], halves_w.at[4 * rows : 4 * rows + band, band:]
    ey_h, ey_l = wide_w.at[0:band], wide_w.at[band:]

    loads[0].wait()
    loads[1].wait()
    sum_c = jnp.zeros((rows, half), F32)
    sum_s = jnp.zeros((rows, half), F32)
    row_sum = jnp.zeros((rows, LANES), F32)
    for g in range(chunks // group):
        pieces[g].wait()
        for j in range(group):
            h = g * group + j
            piece = t_ref[:, h * band : (h + 1) * band]
            high, low = split(piece)
            t_h[h * rows : (h + 1) * rows, :] = high
            t_l[h * rows : (h + 1) * rows, :] = low
            row_sum = row_sum + piece[:, :half] + piece[:, half:]
        lo, hi = g * group * rows, (g + 1) * group * rows
        a_h, a_l = t_h[lo:hi, :], t_l[lo:hi, :]
        y = dot(a_h, wy_h[...]) + dot(a_l, wy_h[...]) + dot(a_h, wy_l[...])
        for j in range(group):
            h = g * group + j
            c = y[j * rows : (j + 1) * rows, :half]
            s = y[j * rows : (j + 1) * rows, half:]
            tc, ts = tw_chunk[h : h + 1, :half], tw_chunk[h : h + 1, half:]
            sum_c = sum_c + (c * tc - s * ts)
            sum_s = sum_s + (c * ts + s * tc)
    turned = jnp.transpose(jnp.concatenate([sum_c, sum_s], axis=0))
    column = jnp.sum(row_sum, axis=1, keepdims=True)
    lane = lax.broadcasted_iota(jnp.int32, (rows, LANES), 1)
    row = lax.broadcasted_iota(jnp.int32, (rows, LANES), 0)
    zero_row = jnp.sum(jnp.where(lane == row, column, 0.0), axis=0, keepdims=True)
    z_ref[:, 0:TILE, :] = turned.reshape(blocks, TILE, LANES)
    z_ref[:, TILE : 2 * TILE, :] = jnp.broadcast_to(zero_row[None], (blocks, TILE, LANES))

    pl.semaphore_wait(barrier, count)

    first = []
    for step in sorted(range(1 - reach, reach + 1), key=lambda d: -abs(d)):
        for other in (False, True):
            if not (step or other):
                continue
            n = len(first)
            copy = pltpu.make_async_remote_copy(
                src_ref=z_ref.at[residue(step, other), pl.ds(0, TILE + 1)],
                dst_ref=slots.at[2 * (reach - step) + core, pl.ds(0, TILE + 1)],
                send_sem=s1.at[n],
                recv_sem=r1.at[n],
                device_id={"slab": at(step, other)},
                device_id_type=MESH,
            )
            copy.start()
            first.append(copy)
    pl.semaphore_signal(rel, inc=1, device_id={"slab": at(-reach)}, device_id_type=MESH)

    slots[2 * reach + core] = z_ref[own]

    own_tw = tw_slab[pl.ds(me, 1), :]
    c0, s0 = own_tw[:, :half], own_tw[:, half:]
    ce, se = e_local[:, :half], e_local[:, half:]
    e_own = jnp.concatenate([ce * c0 - se * s0, se * c0 + ce * s0], axis=1)
    high, low = split(e_own)
    e_h[...] = high
    e_l[...] = low

    base = tw_slab[pl.ds(lax.rem(2 * (chip - reach) + slabs, slabs), 1), :]
    bc, bs = base[:, :half], base[:, half:]
    sc, ss = tw_slab[0:blocks, :half], tw_slab[0:blocks, half:]
    wc, ws = bc * sc - bs * ss, bc * ss + bs * sc

    onehot = (lax.broadcasted_iota(jnp.int32, (TILE, band), 1) == half).astype(BF16)
    lane1 = lax.broadcasted_iota(jnp.int32, (1, LANES), 1)
    k_zero[...] = jnp.zeros_like(k_zero)

    def fold_one(k, carry):
        for c in range(2):
            plane = k_raw[k, c]
            p_h, p_l = split(plane)
            v_h, v_l = split(dot(fold[...], p_h) + dot(fold[...], p_l))
            u = dot(v_h, fold_t[...]) + dot(v_l, fold_t[...])
            pp, pm = u[:half, :half], u[:half, half:]
            mp, mm = u[half:, :half], u[half:, half:]
            k_fold[k, c] = pp + mm
            k_fold[k, 2 + c] = pp - mm
            k_fold[k, 4 + c] = mp + pm
            k_fold[k, 6 + c] = mp - pm
            mid = k_raw[k, c, half : half + TILE, :]
            m_h, m_l = split(mid)
            k_row[c, pl.ds(k, 1), :] = (dot(m_h, fold_t[...]) + dot(m_l, fold_t[...]))[0:1]
            n_h, n_l = split(dot_t(onehot, p_h) + dot_t(onehot, p_l))
            k_col[c, pl.ds(k, 1), :] = (dot(n_h, fold_t[...]) + dot(n_l, fold_t[...]))[0:1]
            k_zero[c, 0:1, :] = k_zero[c, 0:1, :] + jnp.where(lane1 == k, mid[0:1, half : half + 1], 0.0)
        return carry

    for copy in loads[2:]:
        copy.wait()
    cuts = (0, nk // 4, nk // 4 + (5 * nk) // 12, nk)
    lax.fori_loop(cuts[0], cuts[1], fold_one, 0)

    for copy in first:
        copy.wait_recv()

    everything = slots[...]
    a_h, a_l = split(everything.reshape(blocks * 2 * TILE, LANES))
    y = dot(a_h, w2_h[...]) + dot(a_l, w2_h[...]) + dot(a_h, w2_l[...])
    cc = jnp.zeros((2 * TILE, half), F32)
    cs = jnp.zeros((2 * TILE, half), F32)
    sc2 = jnp.zeros((TILE, half), F32)
    ss2 = jnp.zeros((TILE, half), F32)
    total = jnp.zeros((2 * TILE, LANES), F32)
    for s in range(blocks):
        lo = s * 2 * TILE
        c, n = y[lo : lo + 2 * TILE, :half], y[lo : lo + 2 * TILE, half:band]
        c2, n2 = y[lo : lo + TILE, band : band + half], y[lo : lo + TILE, band + half :]
        tc, ts = wc[s : s + 1], ws[s : s + 1]
        cc = cc + (c * tc - n * ts)
        cs = cs + (c * ts + n * tc)
        sc2 = sc2 + (c2 * tc - n2 * ts)
        ss2 = ss2 + (c2 * ts + n2 * tc)
        total = total + everything[s]
    lane = lax.broadcasted_iota(jnp.int32, (TILE, LANES), 1)
    row = lax.broadcasted_iota(jnp.int32, (TILE, LANES), 0)
    left = lane < rows
    col_c = jnp.sum(jnp.where(left, total[:TILE], 0.0), axis=1, keepdims=True)
    col_s = jnp.sum(jnp.where(left, 0.0, total[:TILE]), axis=1, keepdims=True)
    both = jnp.sum(jnp.where(left, total[TILE:], 0.0), axis=1, keepdims=True)
    spot = lane == row + TILE * own
    row_c = jnp.sum(jnp.where(spot, col_c, 0.0), axis=0, keepdims=True)
    row_s = jnp.sum(jnp.where(spot, col_s, 0.0), axis=0, keepdims=True)
    extra = jnp.where(row == 0, row_c, 0.0)
    extra = jnp.where(row == 1, row_s, extra)
    extra = jnp.where(row == 2, cc[TILE : TILE + 1], extra)
    extra = jnp.where(row == 3, cs[TILE : TILE + 1], extra)
    extra = jnp.where(row == 4, both[0:1], extra)
    part[0:8, :] = cc[:TILE]
    part[8:16, :] = cs[:TILE]
    part[16:24, :] = sc2
    part[24:32, :] = ss2
    part[32:40, :] = extra

    pl.semaphore_wait(rel, 1)
    spans = ((0, SPLIT_ROW), (SPLIT_ROW, PART_ROWS - SPLIT_ROW))
    second = []
    for turn in range(2):
        for i, step in enumerate((near, -near)):
            span = spans[i] if turn == 0 else spans[1 - i]
            copy = pltpu.make_async_remote_copy(
                src_ref=part.at[pl.ds(*span)],
                dst_ref=pair.at[i, pl.ds(*span)],
                send_sem=s2.at[2 * turn + i],
                recv_sem=r2.at[2 * turn + i],
                device_id={"slab": at(step)},
                device_id_type=MESH,
            )
            copy.start()
            second.append(copy)

    lax.fori_loop(cuts[1], cuts[2], fold_one, 0)

    for i, step in enumerate((near, -near)):
        second[i].wait_recv()
        copy = pltpu.make_async_remote_copy(
            src_ref=pair.at[i, pl.ds(*spans[i])],
            dst_ref=far.at[pl.ds(*spans[i])],
            send_sem=s2.at[4 + i],
            recv_sem=r2.at[4 + i],
            device_id={"slab": at(step)},
            device_id_type=MESH,
        )
        copy.start()
        second.append(copy)

    lax.fori_loop(cuts[2], cuts[3], fold_one, 0)

    for copy in second[2:]:
        copy.wait_recv()
    block = (((part[...] + pair[0]) + pair[1]) + far[...]) * norm
    gath[own] = block

    third, across = [], []

    def cross(slot):
        n = len(across)
        copy = pltpu.make_async_remote_copy(
            src_ref=gath.at[slot, pl.ds(0, 34)],
            dst_ref=gath.at[slot, pl.ds(0, 34)],
            send_sem=sf.at[n],
            recv_sem=rf.at[n],
            device_id={"slab": at(0, True)},
            device_id_type=MESH,
        )
        copy.start()
        across.append(copy)

    order = sorted((d for d in range(1 - reach, reach + 1) if d), key=lambda d: -abs(d))
    for i, step in enumerate(order):
        copy = pltpu.make_async_remote_copy(
            src_ref=gath.at[own, pl.ds(0, 34)],
            dst_ref=gath.at[own, pl.ds(0, 34)],
            send_sem=s3.at[i],
            recv_sem=r3.at[i],
            device_id={"slab": at(step)},
            device_id_type=MESH,
        )
        copy.start()
        third.append(copy)
    cross(own)

    r0, i0, s00 = block[34:35], -block[35:36], block[36:37]
    e_hi, e_lo = e_h[...], e_l[...]
    ur, ui = (k_col[c, :, :half] + k_col[c, :, half:] for c in range(2))
    vr, vi = (k_col[c, :, :half] - k_col[c, :, half:] for c in range(2))
    columns = (
        jnp.concatenate([ur * r0 - vi * i0, -(vi * r0 + ur * i0)], axis=1),
        jnp.concatenate([ui * r0 + vr * i0, vr * r0 - ui * i0], axis=1),
    )
    for c in range(2):
        p_h, p_l = split(columns[c])
        l0 = dot_t(e_hi, p_h) + dot_t(e_lo, p_h) + dot_t(e_hi, p_l)
        l0 = l0 + (k_zero[c, 0:1, :] * s00)[:, : l0.shape[1]]
        for k in range(nk):
            l_zero[k, c] = jnp.broadcast_to(l0[:, k : k + 1], l_zero.shape[2:])

    for i in reversed(range(len(order))):
        third[i].wait_recv()
        cross(residue(-order[i]))
    for copy in across:
        copy.wait_recv()

    planes = [gath[:, i * TILE : (i + 1) * TILE, :].reshape(half, half) for i in range(4)]
    re1 = jnp.transpose(planes[0] - planes[3])
    im1 = -jnp.transpose(planes[1] + planes[2])
    re2 = jnp.transpose(planes[0] + planes[3])
    im2 = jnp.transpose(planes[1] - planes[2])
    edges = jnp.sum(gath[:, 4 * TILE : 5 * TILE, :], axis=0)
    r0, i0 = edges[0:1], -edges[1:2]
    ur, ui = (k_row[c, :, :half] + k_row[c, :, half:] for c in range(2))
    vr, vi = (k_row[c, :, :half] - k_row[c, :, half:] for c in range(2))
    p_zero[0] = jnp.concatenate([ur * r0 - vi * i0, -(vi * r0 + ur * i0)], axis=1)
    p_zero[1] = jnp.concatenate([ui * r0 + vr * i0, vr * r0 - ui * i0], axis=1)
    high_rows = e_h.shape[0]

    def products(k):
        ur1, ui1, vr1, vi1 = k_fold[k, 0], k_fold[k, 1], k_fold[k, 2], k_fold[k, 3]
        ur2, ui2, vr2, vi2 = k_fold[k, 4], k_fold[k, 5], k_fold[k, 6], k_fold[k, 7]
        a1r, a1i = ur1 * re1 - vi1 * im1, ui1 * re1 + vr1 * im1
        a2r, a2i = ur2 * re2 - vi2 * im2, ui2 * re2 + vr2 * im2
        b1r, b1i = vr1 * re1 - ui1 * im1, vi1 * re1 + ur1 * im1
        b2r, b2i = vr2 * re2 - ui2 * im2, vi2 * re2 + ur2 * im2
        places = (
            (0, 0, a1r + a2r), (0, half, -(b1i + b2i)), (half, 0, b2i - b1i), (half, half, a2r - a1r),
            (0, band, a1i + a2i), (0, band + half, b1r + b2r), (half, band, b1r - b2r),
            (half, band + half, a2i - a1i),
        )
        for r, c, value in places:
            high, low = split(value)
            q_h[k, r : r + half, c : c + half] = high
            q_l[k, r : r + half, c : c + half] = low

    def over_x(k):
        w = dot(e_h[...], q_h[k]) + dot(e_l[...], q_h[k]) + dot(e_h[...], q_l[k])
        l_re = w[:, :band] + p_zero[0, k : k + 1, :]
        l_im = w[:, band:] + p_zero[1, k : k + 1, :]
        high, low = split(jnp.concatenate([l_re, l_im], axis=0))
        l_h[k] = high
        l_l[k] = low

    def over_y(k):
        f = dot(l_h[k], ey_h[...]) + dot(l_l[k], ey_h[...]) + dot(l_h[k], ey_l[...])
        for i in range(acc.shape[1] // LANES):
            at_lanes = slice(i * LANES, (i + 1) * LANES)
            f_re = f[:high_rows, at_lanes] + l_zero[k, 0]
            f_im = f[high_rows:, at_lanes] + l_zero[k, 1]
            power = f_re * f_re + f_im * f_im
            acc[:, at_lanes] = acc[:, at_lanes] + power if k else power

    for k in range(nk + 2):
        if k < nk:
            products(k)
        if 0 <= k - 1 < nk:
            over_x(k - 1)
        if k >= 2:
            over_y(k - 2)

    down = sum(w * acc[i : i + rows, :] for i, w in enumerate(binomial))
    image = sum(w * down[:, i : i + COLS] for i, w in enumerate(binomial))
    out_ref[...] = image * (1.0 / nk)

    for copy in first + second + third + across:
        copy.wait_send()


def tables(slabs, side, band, rows, dtype=np.float32):
    half = band // 2
    f = np.arange(1, half + 1)

    def waves(positions):
        angle = (2.0 * math.pi / side) * np.mod(np.outer(positions, f), side)
        return np.concatenate([np.cos(angle), np.sin(angle)], axis=1)

    def halves(x):
        high = x.astype(np.float32).astype(BF16)
        return high, (x - high.astype(np.float64)).astype(BF16)

    local_w = waves(np.arange(band))
    w2 = np.zeros((2 * rows, 2 * band))
    w2[:rows, :band] = local_w[:rows]
    w2[rows:, band:] = local_w[:rows]
    edge_rows = -(-(rows + 4) // 8) * 8
    columns = np.zeros((band, -(-(COLS + 4) // LANES) * LANES))
    columns[:, : COLS + 4] = waves(np.arange(COLS + 4) - 2).T
    fold = np.zeros((band, band), np.float32)
    for i in range(half):
        if i + 1 < half:
            fold[i, half + 1 + i] = 1.0
        fold[half + i, half - 1 - i] = 1.0
    plain = np.concatenate(
        [waves(band * np.arange(side // band)), waves(rows * np.arange(slabs)), waves(np.arange(edge_rows) - 2)]
    ).astype(np.float32)
    folds = np.concatenate([fold, fold.T], axis=1).astype(BF16)
    return (
        plain,
        np.concatenate(halves(local_w)),
        np.concatenate([*halves(w2), folds]),
        np.concatenate(halves(columns)),
    )


def local(transmission, kernel_spectra):
    rows, side = transmission.shape
    nk, _, band, _ = kernel_spectra.shape
    slabs = lax.axis_size("slab")
    half = band // 2
    blocks = half // TILE
    constants = tables(slabs, side, band, rows)
    edge_rows = constants[0].shape[0] - slabs - side // band
    wide = constants[3].shape[1]
    nk_pad = -(-nk // 8) * 8
    vmem = pl.BlockSpec(memory_space=pltpu.VMEM)
    sends1, sends3 = blocks - 1, blocks // 2 - 1
    dma = pltpu.SemaphoreType.DMA
    return pl.pallas_call(
        functools.partial(image_kernel, (slabs, side, band, nk, rows)),
        out_shape=pltpu.VMEM((rows, COLS), F32),
        in_specs=[pl.BlockSpec(memory_space=pl.ANY)] * (2 + len(constants)),
        out_specs=vmem,
        scratch_shapes=[
            pltpu.VMEM((rows, side), F32),
            *(pltpu.VMEM(c.shape, c.dtype) for c in constants),
            pltpu.VMEM(kernel_spectra.shape, F32),
            pltpu.VMEM((nk, 8, half, half), F32),
            pltpu.VMEM((2, nk_pad, band), F32),
            pltpu.VMEM((2, nk_pad, band), F32),
            pltpu.VMEM((2, TILE, LANES), F32),
            pltpu.VMEM((rows * side // band, band), BF16),
            pltpu.VMEM((rows * side // band, band), BF16),
            pltpu.VMEM((blocks, 2 * TILE, LANES), F32),
            pltpu.VMEM((blocks, 2 * TILE, LANES), F32),
            pltpu.VMEM((5 * TILE, LANES), F32),
            pltpu.VMEM((2, 5 * TILE, LANES), F32),
            pltpu.VMEM((5 * TILE, LANES), F32),
            pltpu.VMEM((blocks, 5 * TILE, LANES), F32),
            pltpu.VMEM((edge_rows, band), BF16),
            pltpu.VMEM((edge_rows, band), BF16),
            pltpu.VMEM((nk, 2, edge_rows, LANES), F32),
            pltpu.VMEM((2, nk_pad, band), F32),
            pltpu.VMEM((nk, band, 2 * band), BF16),
            pltpu.VMEM((nk, band, 2 * band), BF16),
            pltpu.VMEM((nk, 2 * edge_rows, band), BF16),
            pltpu.VMEM((nk, 2 * edge_rows, band), BF16),
            pltpu.VMEM((edge_rows, wide), F32),
            dma((5,)),
            dma((side // band // 4,)),
            dma((sends1,)),
            dma((sends1,)),
            dma((6,)),
            dma((6,)),
            dma((sends3,)),
            dma((sends3,)),
            dma((sends3 + 1,)),
            dma((sends3 + 1,)),
            pltpu.SemaphoreType.REGULAR,
        ],
        compiler_params=pltpu.CompilerParams(
            collective_id=0, has_side_effects=True, vmem_limit_bytes=60 * 1024 * 1024
        ),
        name="aerial_image",
    )(transmission, kernel_spectra, *constants)


def solution(mesh):
    return jax.shard_map(
        local,
        mesh=mesh,
        in_specs=(P(("tiles", "slab"), None), P()),
        out_specs=P(("tiles", "slab"), None),
        check_vma=False,
    )
```
